32 devices in a mesh: groups: 2 (over x), scan: 16 (over z, y, core).
Axes of the slice: x: 2, y: 2, z: 4, core: 2. Of those that a mesh axis runs over, the one named last changes fastest.
Arguments:
- object_field: float32 [2, 768, 1792], P(None, ('groups', 'scan')), parts along dimension 1, may hold values from -8 to 8
- probe_field: float32 [2, 2048, 256], P(None, 'groups'), parts along dimension 1, may hold values from -3 to 3
- amplitudes: float32 [128, 256, 256], P(('groups', 'scan')), parts along dimension 0, may hold values from 0.2 to 3
- offsets: int32 [128, 2], P(('groups', 'scan')), parts along dimension 0, may hold values from -8 to 1496, as said below
- live_counts: int32 [32], P(('groups', 'scan')), parts along dimension 0, may hold values from 1 to 4, as said below
Outputs:
- new_object: float32 [2, 768, 1792], P(None, ('groups', 'scan')), parts along dimension 1
- new_probe: float32 [2, 2048, 256], P(None, ('groups', 'scan')), parts along dimension 1
The draws below stay inside these ranges and needn't reach their ends.
There are 2 independent parts, one for each index of `groups`. The reference program is written for one: setup_inputs(seed, part) draws one part's arguments, and reference() takes and returns one part's arrays. A program takes and returns all parts, laid end to end along the dimension named above; each array names one. Nothing has to cross between parts.
Inputs may be any that keep to these rules, and one draw needn't show every extreme that they name: Position p lies in scan row p // 16, column p % 16: offsets[p, 0] is within 8 of 96 * (p // 16) and offsets[p, 1] within 8 of 48 + 96 * (p % 16); the first position of every block of 4, except position 63, has offsets[p, 0] = 96 * (p // 16) - 8; the single position 63 has offsets[p, 0] = 96 * (p // 16) + 8. Block b of 4 consecutive positions measures its first live_counts[b]; some block measures all 4 and some only one.
All inputs are finite; a program needn't handle non-finite values.
Results may differ from the reference program's by a relative error of at most 0.0013.
Values sent between devices are 32-bit elements; how exact they have to be, the bound alone decides.
A program may use at most 128 MiB of HBM per device.

```python
import math
import jax
import jax.numpy as jnp
from jax import lax

PATCH = 256
MODES = 4
STEP = 96
JITTER = 8
SIDE = 48
POS_DEV = 4
GRID_COLS = 16
COLS = 1792
OBJ_ROWS = 384
POSITIONS = 64


def draw_object_field(key, part):
    first_key = jax.random.fold_in(key, 11)
    row_place = jnp.arange(OBJ_ROWS, dtype=jnp.float32) / OBJ_ROWS
    rising = 0.5 * jnp.exp(row_place * math.log(3.0))
    values = jax.random.normal(first_key, (2, OBJ_ROWS, COLS), jnp.float32)
    return jnp.clip(values * rising[None, :, None], -8.0, 8.0)


def draw_offsets(key, part):
    position_ids = jnp.arange(POSITIONS, dtype=jnp.int32)
    scan_row = position_ids // GRID_COLS
    scan_col = position_ids % GRID_COLS
    shake = jax.random.randint(jax.random.fold_in(key, 21), (POSITIONS, 2), -JITTER, JITTER + 1).astype(jnp.int32)
    row_shake = jnp.where(position_ids % POS_DEV == 0, -JITTER, shake[:, 0]).astype(jnp.int32)
    row_shake = row_shake.at[POSITIONS - 1].set(JITTER)
    col_shake = shake[:, 1].at[GRID_COLS - 1].set(JITTER)
    top_row = STEP * scan_row + row_shake
    left_col = SIDE + STEP * scan_col + col_shake
    return jnp.stack([top_row, left_col], 1).astype(jnp.int32)


def draw_live_counts(key, part):
    row_count = POSITIONS // POS_DEV
    counts = jax.random.randint(jax.random.fold_in(key, 31), (row_count,), 1, POS_DEV + 1).astype(jnp.int32)
    fullest = jax.random.randint(jax.random.fold_in(key, 32), (), 0, row_count).astype(jnp.int32)
    row_ids = jnp.arange(row_count, dtype=jnp.int32)
    counts = jnp.where(row_ids == fullest, POS_DEV, counts)
    counts = jnp.where(row_ids == (fullest + row_count // 2) % row_count, 1, counts)
    return counts.astype(jnp.int32)


def level_of(key, extent, cuts, low, high):
    level, own = 1.0, jax.random.fold_in(key, 6)
    for axis_at, blocks in cuts:
        steps = jnp.exp(jax.random.uniform(jax.random.fold_in(own, axis_at), (blocks,), jnp.float32, low / len(cuts), high / len(cuts)))
        level = level * jnp.repeat(steps, extent[axis_at] // blocks).reshape([-1 if axis == axis_at else 1 for axis in range(len(extent))])
    return level


def scatter_about(own_key, extent, width, most, kind=jnp.bfloat16):
    values = width * jax.random.normal(own_key, extent, jnp.float32)
    return jnp.clip(values, min=-most, max=most).astype(kind)


def setup_inputs(seed: int = 0, part: int = 0) -> dict:
    keys = jax.random.split(jax.random.key(seed), 6)
    own_keys = jax.random.split(jax.random.fold_in(keys[5], part), 6)
    return {
        "object_field": draw_object_field(jax.random.fold_in(jax.random.fold_in(keys[5], part), 71), part),
        "probe_field": scatter_about(own_keys[1], (2, MODES * PATCH, PATCH), 0.5, 3.0, jnp.float32),
        "amplitudes": jnp.clip(jnp.exp(math.log(3.0) - 2.7080502 * jax.random.uniform(own_keys[2], (POSITIONS, PATCH, PATCH), jnp.float32) ** level_of(own_keys[2], (POSITIONS, PATCH, PATCH), ((0, 16),), -0.2, 0.2)), 0.2, 3.0),
        "offsets": draw_offsets(jax.random.fold_in(jax.random.fold_in(keys[5], part), 71), part),
        "live_counts": draw_live_counts(jax.random.fold_in(jax.random.fold_in(keys[5], part), 71), part),
    }


def dft_tables(length, sine_sign):
    numbers = jnp.arange(length, dtype=jnp.int32)
    product = numbers[:, None] * numbers[None, :] % length
    angles = product.astype(jnp.float32) * (2.0 * math.pi / length)
    scaling = 1.0 / math.sqrt(length)
    cosine = jnp.cos(angles) * scaling
    sine_part = jnp.sin(angles) * (sine_sign * scaling)
    left_table = jnp.stack([jnp.stack([cosine, sine_part], 1), jnp.stack([-sine_part, cosine], 1)], 0).astype(jnp.bfloat16)
    right_table = jnp.stack([jnp.stack([cosine, -sine_part], 1), jnp.stack([sine_part, cosine], 1)], 0).astype(jnp.bfloat16)
    return (left_table, right_table)

def transform(exit_wave, tables):
    left_table, right_table = tables
    half_done = jnp.einsum('dkcm,camn->dakn', left_table.astype(jnp.float32), exit_wave.astype(jnp.float32), precision=lax.Precision.HIGHEST).astype(jnp.bfloat16)
    return jnp.einsum('camn,cndk->damk', half_done.astype(jnp.float32), right_table.astype(jnp.float32), precision=lax.Precision.HIGHEST)

def exit_update(obj_patch, probe_modes, amplitude, forward, inverse):
    probe_re, probe_im = (probe_modes[0], probe_modes[1])
    patch_re, patch_im = (obj_patch[0], obj_patch[1])
    exit_wave = jnp.stack([probe_re * patch_re - probe_im * patch_im, probe_re * patch_im + probe_im * patch_re]).astype(jnp.bfloat16)
    far_field = transform(exit_wave, forward)
    intensity = lax.optimization_barrier(jnp.sum(far_field[0] * far_field[0] + far_field[1] * far_field[1], axis=0))
    factor = amplitude / jnp.maximum(jnp.sqrt(intensity), 0.5) - 1.0
    far_change = (far_field * factor).astype(jnp.bfloat16)
    exit_change = transform(far_change, inverse)
    grad_re = lax.optimization_barrier(jnp.sum(probe_re * exit_change[0] + probe_im * exit_change[1], axis=0))
    grad_im = lax.optimization_barrier(jnp.sum(probe_re * exit_change[1] - probe_im * exit_change[0], axis=0))
    mode_re = patch_re * exit_change[0] + patch_im * exit_change[1]
    mode_im = patch_re * exit_change[1] - patch_im * exit_change[0]
    return (grad_re, grad_im, jnp.stack([mode_re, mode_im]), patch_re * patch_re + patch_im * patch_im)

def reference(object_field, probe_field, amplitudes, offsets, live_counts):
    probe_modes = probe_field.reshape(2, MODES, PATCH, PATCH)
    illum_one = lax.optimization_barrier(jnp.sum(probe_modes[0] ** 2 + probe_modes[1] ** 2, axis=0))
    forward = dft_tables(PATCH, 1.0)
    inverse = dft_tables(PATCH, -1.0)
    padded_rows = OBJ_ROWS + JITTER + PATCH
    padded = jnp.zeros((2, padded_rows, COLS), jnp.float32).at[:, JITTER:JITTER + OBJ_ROWS].set(object_field)
    position_ids = jnp.arange(POSITIONS, dtype=jnp.int32)
    weights = (position_ids % POS_DEV < live_counts[position_ids // POS_DEV]).astype(jnp.float32)
    zero_index = jnp.zeros((), jnp.int32)

    def visit(running, record):
        grad_grid, grad_probe, obj_norm = running
        amplitude, corner, alive_weight = record
        top_row = (corner[0] + JITTER).astype(jnp.int32)
        left_col = corner[1].astype(jnp.int32)
        obj_patch = lax.dynamic_slice(padded, (zero_index, top_row, left_col), (2, PATCH, PATCH))
        grad_re, grad_im, probe_part, norm_part = exit_update(obj_patch, probe_modes, amplitude, forward, inverse)
        contrib = jnp.stack([grad_re, grad_im, illum_one]) * alive_weight
        current = lax.dynamic_slice(grad_grid, (zero_index, top_row, left_col), (3, PATCH, PATCH))
        grad_grid = lax.dynamic_update_slice(grad_grid, current + contrib, (zero_index, top_row, left_col))
        return ((grad_grid, grad_probe + probe_part * alive_weight, obj_norm + norm_part * alive_weight), None)
    start_state = (jnp.zeros((3, padded_rows, COLS), jnp.float32), jnp.zeros((2, MODES, PATCH, PATCH), jnp.float32), jnp.zeros((PATCH, PATCH), jnp.float32))
    (grad_grid, grad_probe, obj_norm), _ = lax.scan(visit, start_state, (amplitudes, offsets, weights))
    grad_grid = grad_grid[:, JITTER:JITTER + OBJ_ROWS]
    obj_step = grad_grid[:2] / (grad_grid[2] + 1.0)
    probe_step = grad_probe / (obj_norm + 1.0)
    sum_uu = jnp.sum((obj_step[0] ** 2 + obj_step[1] ** 2) * grad_grid[2])
    sum_uc = jnp.sum(obj_step[0] * grad_grid[0] + obj_step[1] * grad_grid[1])
    sum_vv = jnp.sum((probe_step[0] ** 2 + probe_step[1] ** 2) * obj_norm)
    sum_vc = jnp.sum(probe_step * grad_probe)
    step_padded = jnp.zeros((2, padded_rows, COLS), jnp.float32).at[:, JITTER:JITTER + OBJ_ROWS].set(obj_step)

    def cross_terms(summed, record):
        corner, alive_weight = record
        top_row = (corner[0] + JITTER).astype(jnp.int32)
        left_col = corner[1].astype(jnp.int32)
        obj_patch = lax.dynamic_slice(padded, (zero_index, top_row, left_col), (2, PATCH, PATCH))
        step_patch = lax.dynamic_slice(step_padded, (zero_index, top_row, left_col), (2, PATCH, PATCH))
        cross_re = step_patch[0] * obj_patch[0] + step_patch[1] * obj_patch[1]
        cross_im = step_patch[0] * obj_patch[1] - step_patch[1] * obj_patch[0]
        return (summed + jnp.stack([cross_re, cross_im]) * alive_weight, None)
    cross_sum, _ = lax.scan(cross_terms, jnp.zeros((2, PATCH, PATCH), jnp.float32), (offsets, weights))
    conj_re = probe_modes[0] * probe_step[0] + probe_modes[1] * probe_step[1]
    conj_im = probe_modes[0] * probe_step[1] - probe_modes[1] * probe_step[0]
    sum_uv = jnp.sum(conj_re * cross_sum[0] - conj_im * cross_sum[1])
    diag_obj = 1.1 * sum_uu + 1e-06
    diag_probe = 1.1 * sum_vv + 1e-06
    determinant = diag_obj * diag_probe - sum_uv * sum_uv
    rate_obj = (sum_uc * diag_probe - sum_uv * sum_vc) / determinant
    rate_probe = (diag_obj * sum_vc - sum_uv * sum_uc) / determinant
    new_object = object_field + rate_obj * obj_step
    new_probe = probe_field + rate_probe * probe_step.reshape(2, MODES * PATCH, PATCH)
    return (new_object, new_probe)
```

```python
import functools
import math

import jax
import jax.numpy as jnp
import numpy as np
from jax import lax
from jax.experimental import pallas as pl
from jax.experimental.pallas import tpu as pltpu
from jax.sharding import PartitionSpec as P

SPLIT = 4
JITTER = 8
SIDE = 48
LANES = 128
VMEM_LIMIT = 60 * 1024 * 1024


class Sizes:
    def __init__(self, devices, strip, columns, patch, positions):
        self.devices = devices
        self.strip = strip
        self.columns = columns
        self.patch = patch
        self.positions = positions
        self.step = SPLIT * strip
        self.slots = 1 + -(-(patch + JITTER) // strip)
        self.window_rows = JITTER + (self.slots - 1) * strip
        self.col_step = self.step * positions
        used = SIDE + self.step * (positions - 1) + JITTER + patch
        self.width = -(-used // LANES) * LANES
        self.rounds = -(-self.slots // SPLIT)
        self.span = patch + LANES


def dft_tables(length):
    numbers = np.arange(length)
    product = numbers[:, None] * numbers[None, :] % length
    angles = product.astype(np.float32) * np.float32(2.0 * math.pi / length)
    scaling = np.float32(1.0 / math.sqrt(length))
    cosine = np.cos(angles) * scaling
    sine = np.sin(angles) * scaling
    first = np.block([[cosine, sine], [-sine, cosine]])
    second = np.block([[cosine, -sine], [sine, cosine]])
    return jnp.asarray(first, jnp.bfloat16), jnp.asarray(second, jnp.bfloat16)


def gather_kernel(sz, field_ref, window_ref, send_sem, recv_sem, local_sem):
    me = lax.axis_index("scan")
    my_row = lax.div(me, SPLIT)
    strip = sz.strip

    def outgoing(round_, part, short):
        slot = lax.rem(me + 1, SPLIT) + SPLIT * round_
        target = (lax.div(me + 1, SPLIT) - round_) * SPLIT + part
        cols = pl.ds(part * sz.col_step, sz.width)
        if short:
            src = field_ref.at[:, pl.ds(strip - JITTER, JITTER), cols]
            dst = window_ref.at[:, pl.ds(0, JITTER), :]
        else:
            first = pl.multiple_of(JITTER + (slot - 1) * strip, 8)
            src = field_ref.at[:, :, cols]
            dst = window_ref.at[:, pl.ds(first, strip), :]
        return slot, target, src, dst

    def each_outgoing(act):
        for round_ in range(sz.rounds):
            slot0 = lax.rem(me + 1, SPLIT) + SPLIT * round_
            row = lax.div(me + 1, SPLIT) - round_
            valid = (row >= 0) & (row < sz.devices // SPLIT) & (slot0 < sz.slots)
            for part in range(SPLIT):
                for short in ([True, False] if round_ == 0 else [False]):
                    match = (slot0 == 0) if short else (slot0 > 0)
                    slot, target, src, dst = outgoing(round_, part, short)

                    @pl.when(valid & match & (target != me))
                    def _(slot=slot, target=target, src=src, dst=dst):
                        act(
                            pltpu.make_async_remote_copy(
                                src_ref=src,
                                dst_ref=dst,
                                send_sem=send_sem.at[round_ * SPLIT + part],
                                recv_sem=recv_sem.at[slot],
                                device_id={"scan": target},
                                device_id_type=pl.DeviceIdType.MESH,
                            )
                        )

    each_outgoing(lambda copy: copy.start())
    own_slot = lax.rem(me, SPLIT) + 1
    own_first = pl.multiple_of(JITTER + (own_slot - 1) * strip, 8)
    own_cols = pl.ds(pl.multiple_of(lax.rem(me, SPLIT) * sz.col_step, LANES), sz.width)
    own = pltpu.make_async_copy(
        field_ref.at[:, :, own_cols], window_ref.at[:, pl.ds(own_first, strip), :], local_sem
    )
    own.start()
    own.wait()
    for slot in range(sz.slots):
        source = my_row * SPLIT - 1 + slot
        first = 0 if slot == 0 else JITTER + (slot - 1) * strip
        rows = JITTER if slot == 0 else strip
        there = (source >= 0) & (source < sz.devices)

        @pl.when(there & (source != me))
        def _(slot=slot, first=first, rows=rows, source=source):
            pltpu.make_async_remote_copy(
                src_ref=field_ref.at[:, pl.ds(0, rows), pl.ds(0, sz.width)],
                dst_ref=window_ref.at[:, pl.ds(first, rows), :],
                send_sem=send_sem.at[0],
                recv_sem=recv_sem.at[slot],
                device_id={"scan": source},
                device_id_type=pl.DeviceIdType.MESH,
            ).wait_recv()

        @pl.when(jnp.logical_not(there))
        def _(first=first, rows=rows):
            window_ref[:, first : first + rows, :] = jnp.zeros((2, rows, sz.width), jnp.float32)

    each_outgoing(lambda copy: copy.wait_send())


def gather_window(sz, field):
    return pl.pallas_call(
        functools.partial(gather_kernel, sz),
        out_shape=jax.ShapeDtypeStruct((2, sz.window_rows, sz.width), jnp.float32),
        in_specs=[pl.BlockSpec(memory_space=pltpu.VMEM)],
        out_specs=pl.BlockSpec(memory_space=pltpu.VMEM),
        scratch_shapes=[
            pltpu.SemaphoreType.DMA((sz.rounds * SPLIT,)),
            pltpu.SemaphoreType.DMA((sz.slots,)),
            pltpu.SemaphoreType.DMA,
        ],
        compiler_params=pltpu.CompilerParams(has_side_effects=True),
        name="gather_window",
    )(field)


def reduce_kernel(sz, grid_ref, out_ref, slot_ref, send_sem, recv_sem, local_sem):
    me = lax.axis_index("scan")
    my_row = lax.div(me, SPLIT)
    my_part = lax.rem(me, SPLIT)
    strip = sz.strip

    def outgoing(slot):
        if slot == 0:
            src = grid_ref.at[:, pl.ds(0, JITTER), :]
            dst = slot_ref.at[0, my_part, :, pl.ds(strip - JITTER, JITTER), :]
        else:
            src = grid_ref.at[:, pl.ds(JITTER + (slot - 1) * strip, strip), :]
            dst = slot_ref.at[slot // SPLIT, my_part]
        return src, dst

    def each_outgoing(act):
        for slot in range(sz.slots):
            target = my_row * SPLIT - 1 + slot
            src, dst = outgoing(slot)

            @pl.when((target >= 0) & (target < sz.devices) & (target != me))
            def _(slot=slot, target=target, src=src, dst=dst):
                act(
                    pltpu.make_async_remote_copy(
                        src_ref=src,
                        dst_ref=dst,
                        send_sem=send_sem.at[slot],
                        recv_sem=recv_sem.at[(slot // SPLIT) * SPLIT + my_part],
                        device_id={"scan": target},
                        device_id_type=pl.DeviceIdType.MESH,
                    )
                )

    each_outgoing(lambda copy: copy.start())
    out_ref[...] = jnp.zeros_like(out_ref)
    for round_ in range(sz.rounds):
        row = lax.div(me + 1, SPLIT) - round_
        slot = lax.rem(me + 1, SPLIT) + SPLIT * round_
        valid = (row >= 0) & (row < sz.devices // SPLIT) & (slot < sz.slots)
        for part in range(SPLIT):
            source = row * SPLIT + part
            cols = slice(part * sz.col_step, part * sz.col_step + sz.width)
            for short in ([True, False] if round_ == 0 else [False]):
                match = (slot == 0) if short else (slot > 0)
                begin = strip - JITTER if short else 0
                rows = strip - begin

                @pl.when(valid & match & (source != me))
                def _(begin=begin, rows=rows, source=source, cols=cols, round_=round_, part=part):
                    pltpu.make_async_remote_copy(
                        src_ref=grid_ref.at[:, pl.ds(0, rows), :],
                        dst_ref=slot_ref.at[round_, part, :, pl.ds(begin, rows), :],
                        send_sem=send_sem.at[0],
                        recv_sem=recv_sem.at[round_ * SPLIT + part],
                        device_id={"scan": source},
                        device_id_type=pl.DeviceIdType.MESH,
                    ).wait_recv()
                    out_ref[:, begin:, cols] += slot_ref[round_, part, :, begin:, :]

            @pl.when(valid & (source == me))
            def _(cols=cols):
                first = pl.multiple_of(JITTER + my_part * strip, 8)
                out_ref[:, :, cols] += grid_ref[:, pl.ds(first, strip), :]

    each_outgoing(lambda copy: copy.wait_send())


def reduce_window(sz, grid):
    return pl.pallas_call(
        functools.partial(reduce_kernel, sz),
        out_shape=jax.ShapeDtypeStruct((3, sz.strip, sz.columns), jnp.float32),
        in_specs=[pl.BlockSpec(memory_space=pltpu.VMEM)],
        out_specs=pl.BlockSpec(memory_space=pltpu.VMEM),
        scratch_shapes=[
            pltpu.VMEM((sz.rounds, SPLIT, 3, sz.strip, sz.width), jnp.float32),
            pltpu.SemaphoreType.DMA((sz.slots,)),
            pltpu.SemaphoreType.DMA((sz.rounds * SPLIT,)),
            pltpu.SemaphoreType.DMA,
        ],
        compiler_params=pltpu.CompilerParams(
            has_side_effects=True, vmem_limit_bytes=VMEM_LIMIT
        ),
        name="reduce_window",
    )(grid)


def back(shift, size):
    return jnp.where(shift == 0, 0, size - shift)


def cut(sz, ref, part, top, left):
    base = pl.multiple_of(left // LANES * LANES, LANES)
    block = ref[part, :, pl.ds(base, sz.span)]
    block = pltpu.roll(block, back(left - base, sz.span), 1)[:, : sz.patch]
    return pltpu.roll(block, back(top, sz.window_rows), 0)[: sz.patch]


def put(sz, ref, part, top, left, value):
    base = pl.multiple_of(left // LANES * LANES, LANES)
    below = jnp.zeros((sz.window_rows - sz.patch, sz.patch), jnp.float32)
    block = pltpu.roll(jnp.concatenate([value, below], 0), top, 0)
    beside = jnp.zeros((sz.window_rows, sz.span - sz.patch), jnp.float32)
    block = pltpu.roll(jnp.concatenate([block, beside], 1), left - base, 1)
    ref[part, :, pl.ds(base, sz.span)] += block


def exit_kernel(
    sz,
    corner_ref,
    live_ref,
    window_ref,
    probe_ref,
    amplitude_ref,
    first_ref,
    second_ref,
    grid_ref,
    grad_ref,
    norm_ref,
    patch_ref,
    far_ref,
    work_ref,
    total_ref,
    illum_ref,
):
    patch = sz.patch
    modes = probe_ref.shape[1]
    grid_ref[...] = jnp.zeros_like(grid_ref)
    grad_ref[...] = jnp.zeros_like(grad_ref)
    norm_ref[...] = jnp.zeros_like(norm_ref)
    illum = jnp.zeros((patch, patch), jnp.float32)
    for mode in range(modes):
        illum = illum + probe_ref[0, mode] ** 2 + probe_ref[1, mode] ** 2
    illum_ref[...] = illum

    def transform(stacked, left, right):
        half = jnp.dot(left[...], stacked, preferred_element_type=jnp.float32)
        half = half.astype(jnp.bfloat16)
        beside = jnp.concatenate([half[:patch], half[patch:]], 1)
        return jnp.dot(beside, right[...], preferred_element_type=jnp.float32)

    def visit(position, carry):
        top = corner_ref[position, 0]
        left = corner_ref[position, 1]
        patch_ref[0] = cut(sz, window_ref, 0, top, left)
        patch_ref[1] = cut(sz, window_ref, 1, top, left)
        norm_ref[...] += patch_ref[0] ** 2 + patch_ref[1] ** 2
        work_ref[...] = jnp.zeros_like(work_ref)

        def ahead(mode, carry):
            obj_re, obj_im = patch_ref[0], patch_ref[1]
            probe_re, probe_im = probe_ref[0, mode], probe_ref[1, mode]
            wave_re = (probe_re * obj_re - probe_im * obj_im).astype(jnp.bfloat16)
            wave_im = (probe_re * obj_im + probe_im * obj_re).astype(jnp.bfloat16)
            far = transform(jnp.concatenate([wave_re, wave_im], 0), first_ref, second_ref)
            far_ref[mode] = far
            work_ref[...] += far[:, :patch] ** 2 + far[:, patch:] ** 2
            return carry

        lax.fori_loop(0, modes, ahead, 0)
        work_ref[...] = (
            amplitude_ref[position] * jnp.minimum(lax.rsqrt(work_ref[...]), 2.0) - 1.0
        )
        total_ref[...] = jnp.zeros_like(total_ref)

        def behind(mode, carry):
            factor = work_ref[...]
            change_re = (far_ref[mode, :, :patch] * factor).astype(jnp.bfloat16)
            change_im = (far_ref[mode, :, patch:] * factor).astype(jnp.bfloat16)
            chi = transform(jnp.concatenate([change_re, change_im], 0), second_ref, first_ref)
            chi_re, chi_im = chi[:, :patch], chi[:, patch:]
            probe_re, probe_im = probe_ref[0, mode], probe_ref[1, mode]
            total_ref[0] += probe_re * chi_re + probe_im * chi_im
            total_ref[1] += probe_re * chi_im - probe_im * chi_re
            obj_re, obj_im = patch_ref[0], patch_ref[1]
            grad_ref[0, mode] += obj_re * chi_re + obj_im * chi_im
            grad_ref[1, mode] += obj_re * chi_im - obj_im * chi_re
            return carry

        lax.fori_loop(0, modes, behind, 0)
        put(sz, grid_ref, 0, top, left, total_ref[0])
        put(sz, grid_ref, 1, top, left, total_ref[1])
        put(sz, grid_ref, 2, top, left, illum_ref[...])
        return carry

    lax.fori_loop(0, live_ref[0], visit, 0)


def exit_update(sz, corners, live, window, probe_modes, amplitudes):
    modes = probe_modes.shape[1]
    patch = sz.patch
    first, second = dft_tables(patch)
    vmem = pl.BlockSpec(memory_space=pltpu.VMEM)
    smem = pl.BlockSpec(memory_space=pltpu.SMEM)
    return pl.pallas_call(
        functools.partial(exit_kernel, sz),
        out_shape=(
            jax.ShapeDtypeStruct((3, sz.window_rows, sz.width), jnp.float32),
            jax.ShapeDtypeStruct((2, modes, patch, patch), jnp.float32),
            jax.ShapeDtypeStruct((patch, patch), jnp.float32),
        ),
        in_specs=[smem, smem] + [vmem] * 5,
        out_specs=(vmem, vmem, vmem),
        scratch_shapes=[
            pltpu.VMEM((2, patch, patch), jnp.float32),
            pltpu.VMEM((modes, patch, 2 * patch), jnp.float32),
            pltpu.VMEM((patch, patch), jnp.float32),
            pltpu.VMEM((2, patch, patch), jnp.float32),
            pltpu.VMEM((patch, patch), jnp.float32),
        ],
        compiler_params=pltpu.CompilerParams(vmem_limit_bytes=VMEM_LIMIT),
        name="exit_update",
    )(corners, live, window, probe_modes, amplitudes, first, second)


def cross_kernel(sz, corner_ref, live_ref, window_ref, step_ref, out_ref):
    out_ref[...] = jnp.zeros_like(out_ref)

    def visit(position, carry):
        top = corner_ref[position, 0]
        left = corner_ref[position, 1]
        obj_re = cut(sz, window_ref, 0, top, left)
        obj_im = cut(sz, window_ref, 1, top, left)
        step_re = cut(sz, step_ref, 0, top, left)
        step_im = cut(sz, step_ref, 1, top, left)
        out_ref[0] += step_re * obj_re + step_im * obj_im
        out_ref[1] += step_re * obj_im - step_im * obj_re
        return carry

    lax.fori_loop(0, live_ref[0], visit, 0)


def cross_terms(sz, corners, live, window, step_window):
    vmem = pl.BlockSpec(memory_space=pltpu.VMEM)
    smem = pl.BlockSpec(memory_space=pltpu.SMEM)
    return pl.pallas_call(
        functools.partial(cross_kernel, sz),
        out_shape=jax.ShapeDtypeStruct((2, sz.patch, sz.patch), jnp.float32),
        in_specs=[smem, smem, vmem, vmem],
        out_specs=vmem,
        compiler_params=pltpu.CompilerParams(vmem_limit_bytes=VMEM_LIMIT),
        name="cross_terms",
    )(corners, live, window, step_window)


def on_device(object_field, probe_field, amplitudes, offsets, live_counts):
    sz = Sizes(
        lax.axis_size("scan"),
        object_field.shape[1],
        object_field.shape[2],
        amplitudes.shape[1],
        amplitudes.shape[0],
    )
    patch = sz.patch
    mode_count = probe_field.shape[1] // patch
    device_index = lax.axis_index("scan")
    origin = jnp.stack(
        [
            device_index // SPLIT * sz.step - JITTER,
            device_index % SPLIT * sz.col_step,
        ]
    ).astype(jnp.int32)
    corners = offsets - origin[None]
    probe_modes = probe_field.reshape(2, mode_count, patch, patch)

    window = gather_window(sz, object_field)
    grad_grid, grad_probe, obj_norm = exit_update(
        sz, corners, live_counts, window, probe_modes, amplitudes
    )
    own_rows = reduce_window(sz, grad_grid)
    obj_step = own_rows[:2] / (own_rows[2] + 1.0)
    part_uu = jnp.sum((obj_step[0] ** 2 + obj_step[1] ** 2) * own_rows[2])
    part_uc = jnp.sum(obj_step[0] * own_rows[0] + obj_step[1] * own_rows[1])
    step_window = gather_window(sz, obj_step)
    cross_sum = cross_terms(sz, corners, live_counts, window, step_window)

    share_rows = probe_field.shape[1] // sz.devices
    row_start = device_index * share_rows
    probe_share = lax.dynamic_slice_in_dim(probe_field, row_start, share_rows, 1)
    summed_probe, summed_norm = lax.psum((grad_probe, obj_norm), "scan")
    probe_step = summed_probe / (summed_norm + 1.0)
    conj_re = probe_modes[0] * probe_step[0] + probe_modes[1] * probe_step[1]
    conj_im = probe_modes[0] * probe_step[1] - probe_modes[1] * probe_step[0]
    part_uv = jnp.sum(conj_re * cross_sum[0] - conj_im * cross_sum[1])
    flat_rows = mode_count * patch
    step_share = lax.dynamic_slice_in_dim(
        probe_step.reshape(2, flat_rows, patch), row_start, share_rows, 1
    )
    grad_share = lax.dynamic_slice_in_dim(
        summed_probe.reshape(2, flat_rows, patch), row_start, share_rows, 1
    )
    norm_flat = jnp.broadcast_to(summed_norm[None], (mode_count, patch, patch)).reshape(
        flat_rows, patch
    )
    norm_share = lax.dynamic_slice_in_dim(norm_flat, row_start, share_rows, 0)
    part_vv = jnp.sum((step_share[0] ** 2 + step_share[1] ** 2) * norm_share)
    part_vc = jnp.sum(step_share * grad_share)
    totals = lax.psum(jnp.stack([part_uu, part_uv, part_vv, part_uc, part_vc]), "scan")
    diag_obj = 1.1 * totals[0] + 1e-06
    diag_probe = 1.1 * totals[2] + 1e-06
    determinant = diag_obj * diag_probe - totals[1] * totals[1]
    rate_obj = (totals[3] * diag_probe - totals[1] * totals[4]) / determinant
    rate_probe = (diag_obj * totals[4] - totals[1] * totals[3]) / determinant
    new_object = object_field + rate_obj * obj_step
    new_probe = probe_share + rate_probe * step_share
    return (new_object, new_probe)


def solution(mesh):
    in_specs = (
        P(None, ("groups", "scan"), None),
        P(None, "groups", None),
        P(("groups", "scan"), None, None),
        P(("groups", "scan"), None),
        P(("groups", "scan")),
    )
    out_specs = (P(None, ("groups", "scan"), None), P(None, ("groups", "scan"), None))
    return jax.shard_map(
        on_device, mesh=mesh, in_specs=in_specs, out_specs=out_specs, check_vma=False
    )
```

```python
import functools
import math

import jax
import jax.numpy as jnp
import numpy as np
from jax import lax
from jax.experimental import pallas as pl
from jax.experimental.pallas import tpu as pltpu
from jax.sharding import PartitionSpec as P

SPLIT = 4
JITTER = 8
SIDE = 48
LANES = 128
VMEM_LIMIT = 60 * 1024 * 1024


class Sizes:
    def __init__(self, devices, strip, columns, patch, positions):
        self.devices = devices
        self.strip = strip
        self.columns = columns
        self.patch = patch
        self.positions = positions
        self.step = SPLIT * strip
        self.slots = 1 + -(-(patch + JITTER) // strip)
        self.window_rows = JITTER + (self.slots - 1) * strip
        self.col_step = self.step * positions
        used = SIDE + self.step * (positions - 1) + JITTER + patch
        self.width = -(-used // LANES) * LANES
        self.rounds = -(-self.slots // SPLIT)
        self.span = patch + LANES


def dft_tables(length):
    numbers = np.arange(length)
    product = numbers[:, None] * numbers[None, :] % length
    angles = product.astype(np.float32) * np.float32(2.0 * math.pi / length)
    scaling = np.float32(1.0 / math.sqrt(length))
    cosine = np.cos(angles) * scaling
    sine = np.sin(angles) * scaling
    first = np.block([[cosine, sine], [-sine, cosine]])
    second = np.block([[cosine, -sine], [sine, cosine]])
    return jnp.asarray(first, jnp.bfloat16), jnp.asarray(second, jnp.bfloat16)


def gather_kernel(sz, field_ref, window_ref, send_sem, recv_sem, local_sem):
    me = lax.axis_index("scan")
    my_row = lax.div(me, SPLIT)
    strip = sz.strip

    def outgoing(round_, part, short):
        slot = lax.rem(me + 1, SPLIT) + SPLIT * round_
        target = (lax.div(me + 1, SPLIT) - round_) * SPLIT + part
        cols = pl.ds(part * sz.col_step, sz.width)
        if short:
            src = field_ref.at[:, pl.ds(strip - JITTER, JITTER), cols]
            dst = window_ref.at[:, pl.ds(0, JITTER), :]
        else:
            first = pl.multiple_of(JITTER + (slot - 1) * strip, 8)
            src = field_ref.at[:, :, cols]
            dst = window_ref.at[:, pl.ds(first, strip), :]
        return slot, target, src, dst

    def each_outgoing(act):
        for round_ in range(sz.rounds):
            slot0 = lax.rem(me + 1, SPLIT) + SPLIT * round_
            row = lax.div(me + 1, SPLIT) - round_
            valid = (row >= 0) & (row < sz.devices // SPLIT) & (slot0 < sz.slots)
            for part in range(SPLIT):
                for short in ([True, False] if round_ == 0 else [False]):
                    match = (slot0 == 0) if short else (slot0 > 0)
                    slot, target, src, dst = outgoing(round_, part, short)

                    @pl.when(valid & match & (target != me))
                    def _(slot=slot, target=target, src=src, dst=dst):
                        act(
                            pltpu.make_async_remote_copy(
                                src_ref=src,
                                dst_ref=dst,
                                send_sem=send_sem.at[round_ * SPLIT + part],
                                recv_sem=recv_sem.at[slot],
                                device_id={"scan": target},
                                device_id_type=pl.DeviceIdType.MESH,
                            )
                        )

    each_outgoing(lambda copy: copy.start())
    own_slot = lax.rem(me, SPLIT) + 1
    own_first = pl.multiple_of(JITTER + (own_slot - 1) * strip, 8)
    own_cols = pl.ds(pl.multiple_of(lax.rem(me, SPLIT) * sz.col_step, LANES), sz.width)
    own = pltpu.make_async_copy(
        field_ref.at[:, :, own_cols], window_ref.at[:, pl.ds(own_first, strip), :], local_sem
    )
    own.start()
    own.wait()
    for slot in range(sz.slots):
        source = my_row * SPLIT - 1 + slot
        first = 0 if slot == 0 else JITTER + (slot - 1) * strip
        rows = JITTER if slot == 0 else strip
        there = (source >= 0) & (source < sz.devices)

        @pl.when(there & (source != me))
        def _(slot=slot, first=first, rows=rows, source=source):
            pltpu.make_async_remote_copy(
                src_ref=field_ref.at[:, pl.ds(0, rows), pl.ds(0, sz.width)],
                dst_ref=window_ref.at[:, pl.ds(first, rows), :],
                send_sem=send_sem.at[0],
                recv_sem=recv_sem.at[slot],
                device_id={"scan": source},
                device_id_type=pl.DeviceIdType.MESH,
            ).wait_recv()

        @pl.when(jnp.logical_not(there))
        def _(first=first, rows=rows):
            window_ref[:, first : first + rows, :] = jnp.zeros((2, rows, sz.width), jnp.float32)

    each_outgoing(lambda copy: copy.wait_send())


def gather_window(sz, field):
    return pl.pallas_call(
        functools.partial(gather_kernel, sz),
        out_shape=jax.ShapeDtypeStruct((2, sz.window_rows, sz.width), jnp.float32),
        in_specs=[pl.BlockSpec(memory_space=pltpu.VMEM)],
        out_specs=pl.BlockSpec(memory_space=pltpu.VMEM),
        scratch_shapes=[
            pltpu.SemaphoreType.DMA((sz.rounds * SPLIT,)),
            pltpu.SemaphoreType.DMA((sz.slots,)),
            pltpu.SemaphoreType.DMA,
        ],
        compiler_params=pltpu.CompilerParams(has_side_effects=True),
        name="gather_window",
    )(field)


def reduce_kernel(sz, grid_ref, out_ref, slot_ref, send_sem, recv_sem, local_sem):
    me = lax.axis_index("scan")
    my_row = lax.div(me, SPLIT)
    my_part = lax.rem(me, SPLIT)
    strip = sz.strip

    def outgoing(slot):
        if slot == 0:
            src = grid_ref.at[:, pl.ds(0, JITTER), :]
            dst = slot_ref.at[0, my_part, :, pl.ds(strip - JITTER, JITTER), :]
        else:
            src = grid_ref.at[:, pl.ds(JITTER + (slot - 1) * strip, strip), :]
            dst = slot_ref.at[slot // SPLIT, my_part]
        return src, dst

    def each_outgoing(act):
        for slot in range(sz.slots):
            target = my_row * SPLIT - 1 + slot
            src, dst = outgoing(slot)

            @pl.when((target >= 0) & (target < sz.devices) & (target != me))
            def _(slot=slot, target=target, src=src, dst=dst):
                act(
                    pltpu.make_async_remote_copy(
                        src_ref=src,
                        dst_ref=dst,
                        send_sem=send_sem.at[slot],
                        recv_sem=recv_sem.at[(slot // SPLIT) * SPLIT + my_part],
                        device_id={"scan": target},
                        device_id_type=pl.DeviceIdType.MESH,
                    )
                )

    each_outgoing(lambda copy: copy.start())
    out_ref[...] = jnp.zeros_like(out_ref)
    for round_ in range(sz.rounds):
        row = lax.div(me + 1, SPLIT) - round_
        slot = lax.rem(me + 1, SPLIT) + SPLIT * round_
        valid = (row >= 0) & (row < sz.devices // SPLIT) & (slot < sz.slots)
        for part in range(SPLIT):
            source = row * SPLIT + part
            cols = slice(part * sz.col_step, part * sz.col_step + sz.width)
            for short in ([True, False] if round_ == 0 else [False]):
                match = (slot == 0) if short else (slot > 0)
                begin = strip - JITTER if short else 0
                rows = strip - begin

                @pl.when(valid & match & (source != me))
                def _(begin=begin, rows=rows, source=source, cols=cols, round_=round_, part=part):
                    pltpu.make_async_remote_copy(
                        src_ref=grid_ref.at[:, pl.ds(0, rows), :],
                        dst_ref=slot_ref.at[round_, part, :, pl.ds(begin, rows), :],
                        send_sem=send_sem.at[0],
                        recv_sem=recv_sem.at[round_ * SPLIT + part],
                        device_id={"scan": source},
                        device_id_type=pl.DeviceIdType.MESH,
                    ).wait_recv()
                    out_ref[:, begin:, cols] += slot_ref[round_, part, :, begin:, :]

            @pl.when(valid & (source == me))
            def _(cols=cols):
                first = pl.multiple_of(JITTER + my_part * strip, 8)
                out_ref[:, :, cols] += grid_ref[:, pl.ds(first, strip), :]

    each_outgoing(lambda copy: copy.wait_send())


def reduce_window(sz, grid):
    return pl.pallas_call(
        functools.partial(reduce_kernel, sz),
        out_shape=jax.ShapeDtypeStruct((3, sz.strip, sz.columns), jnp.float32),
        in_specs=[pl.BlockSpec(memory_space=pltpu.VMEM)],
        out_specs=pl.BlockSpec(memory_space=pltpu.VMEM),
        scratch_shapes=[
            pltpu.VMEM((sz.rounds, SPLIT, 3, sz.strip, sz.width), jnp.float32),
            pltpu.SemaphoreType.DMA((sz.slots,)),
            pltpu.SemaphoreType.DMA((sz.rounds * SPLIT,)),
            pltpu.SemaphoreType.DMA,
        ],
        compiler_params=pltpu.CompilerParams(
            has_side_effects=True, vmem_limit_bytes=VMEM_LIMIT
        ),
        name="reduce_window",
    )(grid)


def back(shift, size):
    return jnp.where(shift == 0, 0, size - shift)


def cut(sz, ref, part, top, left):
    base = pl.multiple_of(left // LANES * LANES, LANES)
    block = ref[part, :, pl.ds(base, sz.span)]
    block = pltpu.roll(block, back(left - base, sz.span), 1)[:, : sz.patch]
    return pltpu.roll(block, back(top, sz.window_rows), 0)[: sz.patch]


def put(sz, ref, part, top, left, value):
    base = pl.multiple_of(left // LANES * LANES, LANES)
    below = jnp.zeros((sz.window_rows - sz.patch, sz.patch), jnp.float32)
    block = pltpu.roll(jnp.concatenate([value, below], 0), top, 0)
    beside = jnp.zeros((sz.window_rows, sz.span - sz.patch), jnp.float32)
    block = pltpu.roll(jnp.concatenate([block, beside], 1), left - base, 1)
    ref[part, :, pl.ds(base, sz.span)] += block


def exit_kernel(
    sz,
    corner_ref,
    live_ref,
    window_ref,
    probe_ref,
    amplitude_ref,
    first_ref,
    second_ref,
    grid_ref,
    grad_ref,
    norm_ref,
    patch_ref,
    far_ref,
    work_ref,
    total_ref,
    illum_ref,
):
    patch = sz.patch
    modes = probe_ref.shape[1]
    grid_ref[...] = jnp.zeros_like(grid_ref)
    grad_ref[...] = jnp.zeros_like(grad_ref)
    norm_ref[...] = jnp.zeros_like(norm_ref)
    illum = jnp.zeros((patch, patch), jnp.float32)
    for mode in range(modes):
        illum = illum + probe_ref[0, mode] ** 2 + probe_ref[1, mode] ** 2
    illum_ref[...] = illum

    def transform(stacked, left, right):
        half = jnp.dot(left[...], stacked, preferred_element_type=jnp.float32)
        half = half.astype(jnp.bfloat16)
        beside = jnp.concatenate([half[:patch], half[patch:]], 1)
        return jnp.dot(beside, right[...], preferred_element_type=jnp.float32)

    def visit(position, carry):
        top = corner_ref[position, 0]
        left = corner_ref[position, 1]
        patch_ref[0] = cut(sz, window_ref, 0, top, left)
        patch_ref[1] = cut(sz, window_ref, 1, top, left)
        norm_ref[...] += patch_ref[0] ** 2 + patch_ref[1] ** 2
        work_ref[...] = jnp.zeros_like(work_ref)

        def ahead(mode, carry):
            obj_re, obj_im = patch_ref[0], patch_ref[1]
            probe_re, probe_im = probe_ref[0, mode], probe_ref[1, mode]
            wave_re = (probe_re * obj_re - probe_im * obj_im).astype(jnp.bfloat16)
            wave_im = (probe_re * obj_im + probe_im * obj_re).astype(jnp.bfloat16)
            far = transform(jnp.concatenate([wave_re, wave_im], 0), first_ref, second_ref)
            far_ref[mode] = far
            work_ref[...] += far[:, :patch] ** 2 + far[:, patch:] ** 2
            return carry

        lax.fori_loop(0, modes, ahead, 0)
        work_ref[...] = (
            amplitude_ref[position] * jnp.minimum(lax.rsqrt(work_ref[...]), 2.0) - 1.0
        )
        total_ref[...] = jnp.zeros_like(total_ref)

        def behind(mode, carry):
            factor = work_ref[...]
            change_re = (far_ref[mode, :, :patch] * factor).astype(jnp.bfloat16)
            change_im = (far_ref[mode, :, patch:] * factor).astype(jnp.bfloat16)
            chi = transform(jnp.concatenate([change_re, change_im], 0), second_ref, first_ref)
            chi_re, chi_im = chi[:, :patch], chi[:, patch:]
            probe_re, probe_im = probe_ref[0, mode], probe_ref[1, mode]
            total_ref[0] += probe_re * chi_re + probe_im * chi_im
            total_ref[1] += probe_re * chi_im - probe_im * chi_re
            obj_re, obj_im = patch_ref[0], patch_ref[1]
            grad_ref[0, mode] += obj_re * chi_re + obj_im * chi_im
            grad_ref[1, mode] += obj_re * chi_im - obj_im * chi_re
            return carry

        lax.fori_loop(0, modes, behind, 0)
        put(sz, grid_ref, 0, top, left, total_ref[0])
        put(sz, grid_ref, 1, top, left, total_ref[1])
        put(sz, grid_ref, 2, top, left, illum_ref[...])
        return carry

    lax.fori_loop(0, live_ref[0], visit, 0)


def exit_update(sz, corners, live, window, probe_modes, amplitudes):
    modes = probe_modes.shape[1]
    patch = sz.patch
    first, second = dft_tables(patch)
    vmem = pl.BlockSpec(memory_space=pltpu.VMEM)
    smem = pl.BlockSpec(memory_space=pltpu.SMEM)
    return pl.pallas_call(
        functools.partial(exit_kernel, sz),
        out_shape=(
            jax.ShapeDtypeStruct((3, sz.window_rows, sz.width), jnp.float32),
            jax.ShapeDtypeStruct((2, modes, patch, patch), jnp.float32),
            jax.ShapeDtypeStruct((patch, patch), jnp.float32),
        ),
        in_specs=[smem, smem] + [vmem] * 5,
        out_specs=(vmem, vmem, vmem),
        scratch_shapes=[
            pltpu.VMEM((2, patch, patch), jnp.float32),
            pltpu.VMEM((modes, patch, 2 * patch), jnp.float32),
            pltpu.VMEM((patch, patch), jnp.float32),
            pltpu.VMEM((2, patch, patch), jnp.float32),
            pltpu.VMEM((patch, patch), jnp.float32),
        ],
        compiler_params=pltpu.CompilerParams(vmem_limit_bytes=VMEM_LIMIT),
        name="exit_update",
    )(corners, live, window, probe_modes, amplitudes, first, second)


def cross_kernel(sz, corner_ref, live_ref, window_ref, step_ref, out_ref):
    out_ref[...] = jnp.zeros_like(out_ref)

    def visit(position, carry):
        top = corner_ref[position, 0]
        left = corner_ref[position, 1]
        obj_re = cut(sz, window_ref, 0, top, left)
        obj_im = cut(sz, window_ref, 1, top, left)
        step_re = cut(sz, step_ref, 0, top, left)
        step_im = cut(sz, step_ref, 1, top, left)
        out_ref[0] += step_re * obj_re + step_im * obj_im
        out_ref[1] += step_re * obj_im - step_im * obj_re
        return carry

    lax.fori_loop(0, live_ref[0], visit, 0)


def cross_terms(sz, corners, live, window, step_window):
    vmem = pl.BlockSpec(memory_space=pltpu.VMEM)
    smem = pl.BlockSpec(memory_space=pltpu.SMEM)
    return pl.pallas_call(
        functools.partial(cross_kernel, sz),
        out_shape=jax.ShapeDtypeStruct((2, sz.patch, sz.patch), jnp.float32),
        in_specs=[smem, smem, vmem, vmem],
        out_specs=vmem,
        compiler_params=pltpu.CompilerParams(vmem_limit_bytes=VMEM_LIMIT),
        name="cross_terms",
    )(corners, live, window, step_window)


def total_kernel(devices, part_ref, out_ref, slot_ref, send_sem, recv_sem):
    me = lax.axis_index("scan")

    def copy(distance):
        return pltpu.make_async_remote_copy(
            src_ref=part_ref,
            dst_ref=slot_ref.at[me],
            send_sem=send_sem.at[distance],
            recv_sem=recv_sem.at[distance],
            device_id={"scan": lax.rem(me + distance, devices)},
            device_id_type=pl.DeviceIdType.MESH,
        )

    for distance in range(1, devices):
        copy(distance).start()
    slot_ref[me] = part_ref[...]
    for distance in range(1, devices):
        source = lax.rem(me + devices - distance, devices)
        pltpu.make_async_remote_copy(
            src_ref=part_ref,
            dst_ref=slot_ref.at[source],
            send_sem=send_sem.at[distance],
            recv_sem=recv_sem.at[distance],
            device_id={"scan": source},
            device_id_type=pl.DeviceIdType.MESH,
        ).wait_recv()
    summed = slot_ref[0]
    for source in range(1, devices):
        summed = summed + slot_ref[source]
    out_ref[...] = summed
    for distance in range(1, devices):
        copy(distance).wait_send()


def total_over_scan(devices, parts):
    rows = 8
    padded = jnp.concatenate([parts, jnp.zeros((rows - parts.shape[0],), jnp.float32)])
    return pl.pallas_call(
        functools.partial(total_kernel, devices),
        out_shape=jax.ShapeDtypeStruct((rows, LANES), jnp.float32),
        in_specs=[pl.BlockSpec(memory_space=pltpu.VMEM)],
        out_specs=pl.BlockSpec(memory_space=pltpu.VMEM),
        scratch_shapes=[
            pltpu.VMEM((devices, rows, LANES), jnp.float32),
            pltpu.SemaphoreType.DMA((devices,)),
            pltpu.SemaphoreType.DMA((devices,)),
        ],
        compiler_params=pltpu.CompilerParams(has_side_effects=True),
        name="total_over_scan",
    )(jnp.broadcast_to(padded[:, None], (rows, LANES)))[:, 0]


def on_device(object_field, probe_field, amplitudes, offsets, live_counts):
    sz = Sizes(
        lax.axis_size("scan"),
        object_field.shape[1],
        object_field.shape[2],
        amplitudes.shape[1],
        amplitudes.shape[0],
    )
    patch = sz.patch
    mode_count = probe_field.shape[1] // patch
    device_index = lax.axis_index("scan")
    origin = jnp.stack(
        [
            device_index // SPLIT * sz.step - JITTER,
            device_index % SPLIT * sz.col_step,
        ]
    ).astype(jnp.int32)
    corners = offsets - origin[None]
    probe_modes = probe_field.reshape(2, mode_count, patch, patch)

    window = gather_window(sz, object_field)
    grad_grid, grad_probe, obj_norm = exit_update(
        sz, corners, live_counts, window, probe_modes, amplitudes
    )
    own_rows = reduce_window(sz, grad_grid)
    obj_step = own_rows[:2] / (own_rows[2] + 1.0)
    part_uu = jnp.sum((obj_step[0] ** 2 + obj_step[1] ** 2) * own_rows[2])
    part_uc = jnp.sum(obj_step[0] * own_rows[0] + obj_step[1] * own_rows[1])
    step_window = gather_window(sz, obj_step)
    cross_sum = cross_terms(sz, corners, live_counts, window, step_window)

    share_rows = probe_field.shape[1] // sz.devices
    row_start = device_index * share_rows
    probe_share = lax.dynamic_slice_in_dim(probe_field, row_start, share_rows, 1)
    summed_probe, summed_norm = lax.psum((grad_probe, obj_norm), "scan")
    probe_step = summed_probe / (summed_norm + 1.0)
    conj_re = probe_modes[0] * probe_step[0] + probe_modes[1] * probe_step[1]
    conj_im = probe_modes[0] * probe_step[1] - probe_modes[1] * probe_step[0]
    part_uv = jnp.sum(conj_re * cross_sum[0] - conj_im * cross_sum[1])
    flat_rows = mode_count * patch
    step_share = lax.dynamic_slice_in_dim(
        probe_step.reshape(2, flat_rows, patch), row_start, share_rows, 1
    )
    grad_share = lax.dynamic_slice_in_dim(
        summed_probe.reshape(2, flat_rows, patch), row_start, share_rows, 1
    )
    norm_flat = jnp.broadcast_to(summed_norm[None], (mode_count, patch, patch)).reshape(
        flat_rows, patch
    )
    norm_share = lax.dynamic_slice_in_dim(norm_flat, row_start, share_rows, 0)
    part_vv = jnp.sum((step_share[0] ** 2 + step_share[1] ** 2) * norm_share)
    part_vc = jnp.sum(step_share * grad_share)
    totals = total_over_scan(
        sz.devices, jnp.stack([part_uu, part_uv, part_vv, part_uc, part_vc])
    )
    diag_obj = 1.1 * totals[0] + 1e-06
    diag_probe = 1.1 * totals[2] + 1e-06
    determinant = diag_obj * diag_probe - totals[1] * totals[1]
    rate_obj = (totals[3] * diag_probe - totals[1] * totals[4]) / determinant
    rate_probe = (diag_obj * totals[4] - totals[1] * totals[3]) / determinant
    new_object = object_field + rate_obj * obj_step
    new_probe = probe_share + rate_probe * step_share
    return (new_object, new_probe)


def solution(mesh):
    in_specs = (
        P(None, ("groups", "scan"), None),
        P(None, "groups", None),
        P(("groups", "scan"), None, None),
        P(("groups", "scan"), None),
        P(("groups", "scan")),
    )
    out_specs = (P(None, ("groups", "scan"), None), P(None, ("groups", "scan"), None))
    return jax.shard_map(
        on_device, mesh=mesh, in_specs=in_specs, out_specs=out_specs, check_vma=False
    )
```
